256 devices in a mesh: vox: 64 (over x, z_lo, y, core), load: 4 (over z_hi).
Axes of the slice: x: 4, y: 4, z: 8 (z_hi: 4, z_lo: 2; z = z_hi * 2 + z_lo), core: 2. Of those that a mesh axis runs over, the one named last changes fastest.
Arguments:
- reduced_shape_matrix: bfloat16 [65536, 512], P('vox'), may hold values from -0.25 to 0.25
- young_modulus: float32 [65536], P('vox'), may hold values from 0.5 to 2
- work_stiffening_modulus: float32 [65536], P('vox'), may hold values from 0.2 to 2
- entry_flow_stress: float32 [65536], P('vox'), may hold values from 0.5 to 2
- dilation_factor: float32 [65536], P('vox'), may hold values from 0.5 to 2
- heat_difference: float32 [512], P('load'), may hold values from -4 to 4
- flowing_entry_flags: int32 [65536, 512], P('vox', 'load'), may hold values 0 or 1
- starting_permanent_deformation: float32 [65536, 512], P('vox', 'load'), may hold values from -3 to 3
- starting_weights: float32 [512, 512], P('vox', 'load'), may hold values from -5 to 5
- applied_reduced_vector: float32 [512, 512], P('vox', 'load'), may hold values from -768 to 768
- approx_tangent_inverse: float32 [512, 512], replicated, as said below
Outputs:
- final_mode_coefficients: float32 [512, 512], P('vox', 'load')
- strain_out: float32 [65536, 512], P('vox', 'load')
The draws below stay inside these ranges and needn't reach their ends.
Inputs may be any that keep to these rules, and one draw needn't show every extreme that they name: `approx_tangent_inverse`: it has a positive diagonal.
All inputs are finite; a program needn't handle non-finite values. No bound on the sum of `flowing_entry_flags` on one device may be relied on, other than what follows from the above.
Results may differ from the reference program's by a relative error of at most 0.0013.
Values may be sent and summed in bfloat16 or wider, within the bound.
No kernel may reach another device: no remote copies, remote signals or barrier semaphores. Data moves between devices by JAX's collectives and lax.ppermute only.
A program may use at most 64 MiB of HBM per device.

```python
import math
import jax
import jax.numpy as jnp
from jax import lax

M = 512
ITERS = 3
ROWS = 65536
NUM_HEAT_STEPS = 512


def draw_approx_tangent_inverse(key, part):
    diagonal_random_key, key_off = jax.random.split(jax.random.fold_in(key, 7))
    diag_vals = jnp.exp(jax.random.uniform(diagonal_random_key, (M,), jnp.float32, jnp.log(0.3), jnp.log(0.8)))
    offdiag = jax.random.normal(key_off, (M, M), jnp.float32) * (0.15 / jnp.sqrt(jnp.float32(M)))
    matrix = offdiag + jnp.diag(diag_vals)
    return (matrix * (M / ROWS)).astype(jnp.float32)


def plant(result, key, smallest, top_value):
    shape = result.shape
    index_at = [jax.random.randint(jax.random.fold_in(key, axis), (), 0, shape[axis]) for axis in range(len(shape))]
    result = result.at[tuple(index_at)].set(smallest)
    longest = shape.index(max(shape))
    index_at[longest] = (index_at[longest] + 1) % shape[longest]
    return result.at[tuple(index_at)].set(top_value)


def steps_of(stream_key, extent, cuts, least, high):
    def one(dim, shards_of):
        draws = jax.random.uniform(jax.random.fold_in(jax.random.fold_in(stream_key, 6), dim), (shards_of,), jnp.float32, least / len(cuts), high / len(cuts))
        return jnp.repeat(jnp.exp(draws), extent[dim] // shards_of).reshape((-1,) + (1,) * (len(extent) - dim - 1))

    loudness = one(*cuts[0])
    for cut in cuts[1:]:
        loudness = loudness * one(*cut)
    return loudness


def bell_draw(stream_key, dims, scale, most, cuts=(), kind=jnp.bfloat16):
    values = scale * jax.random.normal(stream_key, dims, jnp.float32)
    if cuts:
        values = values * steps_of(stream_key, dims, cuts, -0.22, 0.18)
    return jnp.clip(values, -most, most).astype(kind)


def setup_inputs(seed: int = 0) -> dict:
    arg_keys = jax.random.split(jax.random.key(seed), 12)
    reduced_shape_matrix = bell_draw(arg_keys[0], (ROWS, M), M ** -0.5, 0.25, ((0, 64),))
    young_modulus = jnp.clip(jnp.exp(math.log(2.0) - 1.3862944 * jax.random.uniform(arg_keys[1], (ROWS,), jnp.float32) ** steps_of(arg_keys[1], (ROWS,), ((0, 64),), -0.2, 0.2)), 0.5, 2.0)
    work_stiffening_modulus = jnp.clip(jnp.exp(math.log(2.0) - 2.3025851 * jax.random.uniform(arg_keys[2], (ROWS,), jnp.float32) ** steps_of(arg_keys[2], (ROWS,), ((0, 64),), -0.2, 0.2)), 0.2, 2.0)
    entry_flow_stress = jnp.clip(jnp.exp(math.log(2.0) - 1.3862944 * jax.random.uniform(arg_keys[3], (ROWS,), jnp.float32) ** steps_of(arg_keys[3], (ROWS,), ((0, 64),), -0.2, 0.2)), 0.5, 2.0)
    dilation_factor = jnp.clip(jnp.exp(math.log(2.0) - 1.3862944 * jax.random.uniform(arg_keys[4], (ROWS,), jnp.float32) ** steps_of(arg_keys[4], (ROWS,), ((0, 64),), -0.2, 0.2)), 0.5, 2.0)
    heat_difference = bell_draw(arg_keys[5], (NUM_HEAT_STEPS,), 1.0, 4.0, ((0, 4),), jnp.float32)
    flowing_entry_flags = plant((jax.random.randint(arg_keys[6], (ROWS, NUM_HEAT_STEPS), 0, 2) < 1).astype(jnp.int32), jax.random.fold_in(arg_keys[6], 1), 0, 1)
    starting_permanent_deformation = bell_draw(arg_keys[7], (ROWS, NUM_HEAT_STEPS), 0.5, 3.0, ((0, 64), (1, 4)), jnp.float32)
    starting_weights = bell_draw(arg_keys[8], (M, NUM_HEAT_STEPS), 1.0, 5.0, ((0, 64), (1, 4)), jnp.float32)
    applied_reduced_vector = bell_draw(arg_keys[9], (M, NUM_HEAT_STEPS), (ROWS // M), 768.0, ((0, 64), (1, 4)), jnp.float32)
    approx_tangent_inverse = draw_approx_tangent_inverse(jax.random.fold_in(arg_keys[11], 71), 0)
    return {"reduced_shape_matrix": reduced_shape_matrix, "young_modulus": young_modulus, "work_stiffening_modulus": work_stiffening_modulus, "entry_flow_stress": entry_flow_stress, "dilation_factor": dilation_factor, "heat_difference": heat_difference, "flowing_entry_flags": flowing_entry_flags, "starting_permanent_deformation": starting_permanent_deformation, "starting_weights": starting_weights, "applied_reduced_vector": applied_reduced_vector, "approx_tangent_inverse": approx_tangent_inverse}


def reference(reduced_shape_matrix, young_modulus, work_stiffening_modulus, entry_flow_stress, dilation_factor, heat_difference, flowing_entry_flags, starting_permanent_deformation, starting_weights, applied_reduced_vector, approx_tangent_inverse):
    xi_now = starting_weights
    plastic = starting_permanent_deformation
    active = flowing_entry_flags.astype(jnp.float32)
    modulus = young_modulus[:, None]
    harden = work_stiffening_modulus[:, None]
    yielded = entry_flow_stress[:, None]
    heating_history = dilation_factor[:, None] * heat_difference[None, :]
    for sweep in range(ITERS):
        strain = jnp.dot(reduced_shape_matrix, xi_now.astype(jnp.bfloat16), preferred_element_type=jnp.float32)
        trial = modulus * (strain - heating_history - plastic)
        excess = trial - yielded * jnp.tanh(trial / yielded)
        increment = active * excess / (modulus + harden)
        plastic = plastic + increment
        stress = (trial - modulus * increment).astype(jnp.bfloat16)
        resid = lax.dot_general(reduced_shape_matrix, stress, (((0,), (0,)), ((), ())), preferred_element_type=jnp.float32) - applied_reduced_vector
        delta = jnp.dot(approx_tangent_inverse, resid, precision=lax.Precision.HIGHEST)
        spread = jnp.sum(delta * delta) / (M * NUM_HEAT_STEPS)
        xi_now = xi_now - delta / (1.0 + spread)
    return xi_now, plastic
```

```python
import jax
import jax.numpy as jnp
from jax import lax
from jax.sharding import Mesh
from jax.sharding import PartitionSpec as P

M = 512
ITERS = 3
VOX = ("x", "zl", "y", "core")
XY = ("x", "y")
RING = ("zl", "load")
SWAP = [(0, 1), (1, 0)]
CHUNK = 16


def split_two(value):
    high = lax.reduce_precision(value, 8, 7)
    return high.astype(jnp.bfloat16), (value - high).astype(jnp.bfloat16)


def dot(a, b, dims):
    return lax.dot_general(a, b, (dims, ((), ())), preferred_element_type=jnp.float32)


def to_everyone(block, axes):
    size = lax.axis_size(axes)
    return lax.all_to_all(
        jnp.broadcast_to(block[None], (size, *block.shape)), axes, 0, 0, tiled=True
    )


def shards(
    reduced_shape_matrix,
    young_modulus,
    work_stiffening_modulus,
    entry_flow_stress,
    dilation_factor,
    heat_difference,
    flowing_entry_flags,
    starting_permanent_deformation,
    starting_weights,
    applied_reduced_vector,
    approx_tangent_inverse,
):
    own_rows, points = starting_weights.shape
    entries = M * points * lax.axis_size("load")
    vox = lax.axis_index(VOX)
    core = lax.axis_index("core")
    load = lax.axis_index("load")
    plastic = starting_permanent_deformation
    active = flowing_entry_flags.astype(jnp.float32)
    modulus = young_modulus[:, None]
    harden = work_stiffening_modulus[:, None]
    yielded = entry_flow_stress[:, None]
    heating_history = dilation_factor[:, None] * heat_difference[None, :]

    xi = to_everyone(starting_weights, VOX).reshape(M, points)

    inverse_high, inverse_low = split_two(approx_tangent_inverse)
    both = dot(inverse_high, reduced_shape_matrix, ((1,), (1,))) + dot(
        inverse_low, reduced_shape_matrix, ((1,), (1,))
    )
    map_high, map_low = split_two(both)
    applied = lax.dynamic_update_slice_in_dim(
        jnp.zeros((M, points), jnp.float32), applied_reduced_vector, vox * own_rows, 0
    )
    applied = jnp.dot(approx_tangent_inverse, applied, precision=lax.Precision.HIGHEST)

    for sweep in range(ITERS):
        strain = dot(reduced_shape_matrix, xi.astype(jnp.bfloat16), ((1,), (0,)))
        trial = modulus * (strain - heating_history - plastic)
        excess = trial - yielded * jnp.tanh(trial / yielded)
        increment = active * excess / (modulus + harden)
        stress = (trial - modulus * increment).astype(jnp.bfloat16)
        plastic = plastic + increment
        partial = dot(map_high, stress, ((1,), (0,))) + dot(map_low, stress, ((1,), (0,))) - applied
        halves = partial.reshape(-1, 2, CHUNK, points)
        kept = lax.dynamic_index_in_dim(halves, core, 1, False)
        given = lax.dynamic_index_in_dim(halves, 1 - core, 1, False)
        kept = kept + lax.ppermute(given, "core", SWAP)
        chunk = jnp.sum(lax.all_to_all(kept, XY, 0, 0, tiled=True), axis=0)
        ring = to_everyone(chunk, RING)
        ring = jnp.sum(ring.reshape(2, -1, CHUNK, points), axis=0)
        squares = jnp.sum(ring * ring)
        delta = lax.dynamic_index_in_dim(ring, load, 0, False)
        message = jnp.concatenate([delta, jnp.full((8, points), squares)], axis=0)
        other = lax.ppermute(message, "core", SWAP)
        pair = jnp.where(core == 0, jnp.stack([message, other]), jnp.stack([other, message]))
        pairs = to_everyone(pair, XY)
        delta = pairs[:, :, :CHUNK].reshape(M, points)
        spread = jnp.sum(pairs[:, :, CHUNK, 0]) / entries
        xi = xi - delta / (1.0 + spread)
    return (lax.dynamic_slice_in_dim(xi, vox * own_rows, own_rows, 0), plastic)


def solution(mesh):
    split = Mesh(
        mesh.devices.reshape(4, 2, 4, 2, mesh.shape["load"]),
        ("x", "zl", "y", "core", "load"),
    )
    return jax.shard_map(
        shards,
        mesh=split,
        in_specs=(
            P(VOX, None),
            P(VOX),
            P(VOX),
            P(VOX),
            P(VOX),
            P("load"),
            P(VOX, "load"),
            P(VOX, "load"),
            P(VOX, "load"),
            P(VOX, "load"),
            P(),
        ),
        out_specs=(P(VOX, "load"), P(VOX, "load")),
        check_vma=False,
    )
```

```python
import functools

import jax
import jax.numpy as jnp
from jax import lax
from jax.experimental import pallas as pl
from jax.experimental.pallas import tpu as pltpu
from jax.sharding import Mesh
from jax.sharding import PartitionSpec as P

M = 512
ITERS = 3
VOX = ("x", "zl", "y", "core")
PLANE = ("x", "y")
COLUMNS = ("x", "y", "core")
RING = ("zl", "load")
SWAP = [(0, 1), (1, 0)]
CHUNK = 16
CHUNKS = M // CHUNK
BLOCK = 128

HERE = pl.BlockSpec(memory_space=pltpu.VMEM)
ANYWHERE = pl.BlockSpec(memory_space=pl.ANY)
SCALAR = pl.BlockSpec(memory_space=pltpu.SMEM)
F32 = jnp.float32
BF16 = jnp.bfloat16


def call(kernel, name, outs, n_scalars, n_arrays, scratch=(), n_unread=0):
    return pl.pallas_call(
        kernel,
        name=name,
        out_shape=[jax.ShapeDtypeStruct(*out) for out in outs],
        in_specs=[SCALAR] * n_scalars + [HERE] * n_arrays + [ANYWHERE] * n_unread,
        out_specs=[HERE] * len(outs),
        scratch_shapes=list(scratch),
        compiler_params=pltpu.CompilerParams(vmem_limit_bytes=16 << 20),
    )


def dot(a, b, dims=((1,), (0,))):
    return lax.dot_general(a, b, (dims, ((), ())), preferred_element_type=F32)


def split_two(value):
    high = value.astype(BF16)
    return high, (value - high.astype(F32)).astype(BF16)


def send_kernel(place, core, load, own, out):
    for peer in range(out.shape[0]):
        out[peer] = own[...]


def prepare_kernel(
    place, inverse, basis, young, harden, flow, dilate, heat, flags, applied, after,
    high_out, low_out, applied_out, young_out, flow_out, inv_flow_out, weight_out, heat_out,
    padded,
):
    inverse_high, inverse_low = split_two(inverse[...])
    for block in range(0, basis.shape[0], 256):
        rows = slice(block, block + 256)
        part = basis[rows, :]
        both = dot(inverse_high, part, ((1,), (1,))) + dot(inverse_low, part, ((1,), (1,)))
        high, low = split_two(both)
        high_out[:, rows] = high
        low_out[:, rows] = low
    padded[...] = jnp.zeros_like(padded)
    padded[pl.ds(pl.multiple_of(place[0] % 16 * 8, 8), 8), :] = applied[...]
    columns = inverse[:, pl.ds(pl.multiple_of(place[0] // 16 * 128, 128), 128)]
    a_high, a_low = split_two(columns)
    b_high, b_low = split_two(padded[...])
    applied_out[...] = dot(a_high, b_high) + (dot(a_high, b_low) + dot(a_low, b_high))
    young_t = young[...].T
    flow_t = flow[...].T
    inv_flow_t = (1.0 / flow[...]).T
    weight_t = (1.0 / (young[...] + harden[...])).T
    dilate_t = dilate[...].T
    for block in range(8):
        rows = slice(block * 128, block * 128 + 128)
        column = slice(block, block + 1)
        wide = (128, 128)
        young_out[rows, :] = jnp.broadcast_to(young_t[:, column], wide)
        flow_out[rows, :] = jnp.broadcast_to(flow_t[:, column], wide)
        inv_flow_out[rows, :] = jnp.broadcast_to(inv_flow_t[:, column], wide)
        weight_out[rows, :] = flags[rows, :].astype(F32) * weight_t[:, column]
        heat_out[rows, :] = dilate_t[:, column] * heat[...]


def factor_of(mine, other, entries):
    squares = mine[0, CHUNK:] + other[0, CHUNK:]
    for peer in range(1, mine.shape[0]):
        squares = squares + mine[peer, CHUNK:] + other[peer, CHUNK:]
    spread = jnp.sum(squares, axis=(0, 1), keepdims=True) / entries
    return 1.0 / (1.0 + spread)


def constitutive(xi_now, basis, high, low, applied, young, flow, inv_flow, weight, heat, plastic, plastic_out, sums_out, stress_all):
    for block in range(0, basis.shape[0], BLOCK):
        rows = slice(block, block + BLOCK)
        strain = dot(basis[rows, :], xi_now)
        trial = young[rows, :] * (strain - heat[rows, :] - plastic[rows, :])
        excess = trial - flow[rows, :] * jnp.tanh(trial * inv_flow[rows, :])
        increment = weight[rows, :] * excess
        plastic_out[rows, :] = plastic[rows, :] + increment
        stress_all[rows, :] = (trial - young[rows, :] * increment).astype(BF16)
    stress = stress_all[...]
    sums_out[...] = dot(high[...], stress) + dot(low[...], stress) - applied[...]


def first_kernel(xi, *rest):
    constitutive(xi[...].reshape(M, -1).astype(BF16), *rest)


def next_kernel(entries, core_ref, mine, other, xi, *rest):
    *rest, xi_out, stress_all, xi_low = rest
    core = core_ref[0]
    factor = factor_of(mine, other, entries)
    for peer in range(mine.shape[0]):
        for source, spot in ((mine, 2 * peer + core), (other, 2 * peer + 1 - core)):
            value = xi[spot] - source[peer, :CHUNK] * factor
            xi_out[spot] = value
            xi_low[spot] = value.astype(BF16)
    constitutive(xi_low[...].reshape(M, -1), *rest, stress_all)


def last_kernel(entries, core_ref, place, mine, other, xi, out):
    factor = factor_of(mine, other, entries)
    chunk = place[0] // 2
    half = pl.ds(pl.multiple_of(place[0] % 2 * 8, 8), 8)
    here = chunk % 2 == core_ref[0]
    delta = jnp.where(here, mine[chunk // 2, half], other[chunk // 2, half])
    out[...] = xi[chunk, half] - delta * factor


def relay_kernel(pieces, out):
    total = pieces[0]
    for peer in range(1, pieces.shape[0]):
        total = total + pieces[peer]
    for peer in range(out.shape[0]):
        out[peer] = total


def close_kernel(load, pieces, out):
    loads = pieces.shape[0] // 2
    squares = jnp.zeros((8, out.shape[2]), F32)
    for group in range(loads):
        total = pieces[group] + pieces[loads + group]
        square = total * total
        squares = squares + square[:8] + square[8:]
    delta = pieces[load[0]] + pieces[loads + load[0]]
    for peer in range(out.shape[0]):
        out[peer, :CHUNK] = delta
        out[peer, CHUNK:] = squares


def shards(
    reduced_shape_matrix,
    young_modulus,
    work_stiffening_modulus,
    entry_flow_stress,
    dilation_factor,
    heat_difference,
    flowing_entry_flags,
    starting_permanent_deformation,
    starting_weights,
    applied_reduced_vector,
    approx_tangent_inverse,
):
    rows, points = starting_permanent_deformation.shape
    own_rows = starting_weights.shape[0]
    size = lax.axis_size
    entries = M * points * size("load")
    place = lax.axis_index(VOX).reshape(1)
    core = lax.axis_index("core").reshape(1)
    load = lax.axis_index("load").reshape(1)
    exchange = functools.partial(lax.all_to_all, split_axis=0, concat_axis=0, tiled=True)

    (weights,) = call(send_kernel, "send", [((size(VOX), own_rows, points), F32)], 3, 1)(
        place, core, load, starting_weights
    )
    xi = exchange(weights, VOX).reshape(CHUNKS, CHUNK, points)

    square = (8, rows // 8)
    wide = ((rows, points), F32)
    fixed = call(
        prepare_kernel,
        "prepare",
        [((M, rows), BF16), ((M, rows), BF16), ((M, points), F32), wide, wide, wide, wide, wide],
        1,
        9,
        [pltpu.VMEM((128, points), F32)],
        1,
    )(
        place,
        approx_tangent_inverse,
        reduced_shape_matrix,
        young_modulus.reshape(square),
        work_stiffening_modulus.reshape(square),
        entry_flow_stress.reshape(square),
        dilation_factor.reshape(square),
        heat_difference.reshape(1, points),
        flowing_entry_flags,
        applied_reduced_vector,
        xi,
    )
    plastic = starting_permanent_deformation
    stress_room = pltpu.VMEM((rows, points), BF16)
    sums_shape = ((M, points), F32)
    xi_shape = ((CHUNKS, CHUNK, points), F32)

    mine = other = None
    for sweep in range(ITERS):
        if sweep == 0:
            plastic, sums = call(first_kernel, "first", [wide, sums_shape], 0, 11, [stress_room])(
                xi, reduced_shape_matrix, *fixed, plastic
            )
        else:
            plastic, sums, xi = call(
                functools.partial(next_kernel, entries),
                "next",
                [wide, sums_shape, xi_shape],
                1,
                13,
                [stress_room, pltpu.VMEM(xi_shape[0], BF16)],
            )(core, mine, other, xi, reduced_shape_matrix, *fixed, plastic)
        pieces = exchange(sums.reshape(CHUNKS, CHUNK, points), COLUMNS)
        (ring,) = call(relay_kernel, "relay", [((size(RING), CHUNK, points), F32)], 0, 1)(pieces)
        ring = exchange(ring, RING)
        (message,) = call(close_kernel, "close", [((size(PLANE), CHUNK + 8, points), F32)], 1, 1)(load, ring)
        mine = exchange(message, PLANE)
        other = lax.ppermute(mine, "core", SWAP)
    (xi_own,) = call(
        functools.partial(last_kernel, entries), "last", [((own_rows, points), F32)], 2, 3
    )(core, place, mine, other, xi)
    return (xi_own, plastic)


def solution(mesh):
    split = Mesh(
        mesh.devices.reshape(4, 2, 4, 2, mesh.shape["load"]),
        ("x", "zl", "y", "core", "load"),
    )
    return jax.shard_map(
        shards,
        mesh=split,
        in_specs=(
            P(VOX, None),
            P(VOX),
            P(VOX),
            P(VOX),
            P(VOX),
            P("load"),
            P(VOX, "load"),
            P(VOX, "load"),
            P(VOX, "load"),
            P(VOX, "load"),
            P(),
        ),
        out_specs=(P(VOX, "load"), P(VOX, "load")),
        check_vma=False,
    )
```

```python
import functools

import jax
import jax.numpy as jnp
from jax import lax
from jax.experimental import pallas as pl
from jax.experimental.pallas import tpu as pltpu
from jax.sharding import Mesh
from jax.sharding import PartitionSpec as P

M = 512
ITERS = 3
VOX = ("x", "zl", "y", "core")
PLANE = ("x", "y")
COLUMNS = ("x", "y", "core")
RING = ("zl", "load")
SWAP = [(0, 1), (1, 0)]
CHUNK = 16
CHUNKS = M // CHUNK
BLOCK = 128

HERE = pl.BlockSpec(memory_space=pltpu.VMEM)
SCALAR = pl.BlockSpec(memory_space=pltpu.SMEM)
F32 = jnp.float32
BF16 = jnp.bfloat16


def call(kernel, name, outs, n_scalars, n_arrays, scratch=()):
    return pl.pallas_call(
        kernel,
        name=name,
        out_shape=[jax.ShapeDtypeStruct(*out) for out in outs],
        in_specs=[SCALAR] * n_scalars + [HERE] * n_arrays,
        out_specs=[HERE] * len(outs),
        scratch_shapes=list(scratch),
        compiler_params=pltpu.CompilerParams(vmem_limit_bytes=16 << 20),
    )


def dot(a, b, dims=((1,), (0,))):
    return lax.dot_general(a, b, (dims, ((), ())), preferred_element_type=F32)


def split_two(value):
    high = value.astype(BF16)
    return high, (value - high.astype(F32)).astype(BF16)


def send_kernel(place, core, load, own, out):
    for peer in range(out.shape[0]):
        out[peer] = own[...]


def prepare_kernel(
    place, inverse, basis, young, harden, flow, dilate, heat, flags, applied, plastic,
    map_out, applied_out, columns_out, heat_out, active_out,
    padded,
):
    inverse_high, inverse_low = split_two(inverse[...])
    for block in range(0, basis.shape[0], 256):
        rows = slice(block, block + 256)
        part = basis[rows, :]
        both = dot(inverse_high, part, ((1,), (1,))) + dot(inverse_low, part, ((1,), (1,)))
        map_out[:, rows] = both.astype(BF16)
    heat_out[...] = heat[...]
    active_out[...] = flags[...].astype(BF16)
    padded[...] = jnp.zeros_like(padded)
    padded[pl.ds(pl.multiple_of(place[0] % 16 * 8, 8), 8), :] = applied[...]
    columns = inverse[:, pl.ds(pl.multiple_of(place[0] // 16 * 128, 128), 128)]
    a_high, a_low = split_two(columns)
    b_high, b_low = split_two(padded[...])
    applied_out[...] = dot(a_high, b_high) + (dot(a_high, b_low) + dot(a_low, b_high))
    factors = (
        young[...] / flow[...],
        flow[...],
        young[...],
        flow[...] / (young[...] + harden[...]),
        dilate[...],
    )
    spare = jnp.zeros((128 - 8 * len(factors), 128), F32)
    columns_out[...] = jnp.concatenate([*factors, spare], axis=0).T


def factor_of(mine, other, entries):
    squares = mine[0, CHUNK:] + other[0, CHUNK:]
    for peer in range(1, mine.shape[0]):
        squares = squares + mine[peer, CHUNK:] + other[peer, CHUNK:]
    spread = jnp.sum(squares, axis=(0, 1), keepdims=True) / entries
    return 1.0 / (1.0 + spread)


def constitutive(xi_now, basis, map_in, applied, columns, heat, active, plastic, plastic_out, sums_out, stress_all):
    for block in range(basis.shape[0] // BLOCK):
        rows = slice(block * BLOCK, block * BLOCK + BLOCK)
        slope, flow, young, weight, dilate = (
            columns[:, 8 * factor + block : 8 * factor + block + 1] for factor in range(5)
        )
        strain = dot(basis[rows, :], xi_now)
        ratio = slope * (strain - dilate * heat[...] - plastic[rows, :])
        increment = active[rows, :].astype(F32) * weight * (ratio - jnp.tanh(ratio))
        plastic_out[rows, :] = plastic[rows, :] + increment
        stress_all[rows, :] = (flow * ratio - young * increment).astype(BF16)
    sums_out[...] = dot(map_in[...], stress_all[...]) - applied[...]


def first_kernel(xi, *rest):
    constitutive(xi[...].reshape(M, -1).astype(BF16), *rest)


def next_kernel(entries, core_ref, mine, other, xi, *rest):
    *rest, xi_out, stress_all, xi_low = rest
    core = core_ref[0]
    factor = factor_of(mine, other, entries)
    for peer in range(mine.shape[0]):
        for source, spot in ((mine, 2 * peer + core), (other, 2 * peer + 1 - core)):
            value = xi[spot] - source[peer, :CHUNK] * factor
            xi_out[spot] = value
            xi_low[spot] = value.astype(BF16)
    constitutive(xi_low[...].reshape(M, -1), *rest, stress_all)


def last_kernel(entries, core_ref, place, mine, other, xi, out):
    factor = factor_of(mine, other, entries)
    chunk = place[0] // 2
    half = pl.ds(pl.multiple_of(place[0] % 2 * 8, 8), 8)
    here = chunk % 2 == core_ref[0]
    delta = jnp.where(here, mine[chunk // 2, half], other[chunk // 2, half])
    out[...] = xi[chunk, half] - delta * factor


def relay_kernel(pieces, out):
    total = pieces[0]
    for peer in range(1, pieces.shape[0]):
        total = total + pieces[peer]
    for peer in range(out.shape[0]):
        out[peer] = total


def close_kernel(load, pieces, out):
    loads = pieces.shape[0] // 2
    squares = jnp.zeros((8, out.shape[2]), F32)
    for group in range(loads):
        total = pieces[group] + pieces[loads + group]
        square = total * total
        squares = squares + square[:8] + square[8:]
    delta = pieces[load[0]] + pieces[loads + load[0]]
    for peer in range(out.shape[0]):
        out[peer, :CHUNK] = delta
        out[peer, CHUNK:] = squares


def shards(
    reduced_shape_matrix,
    young_modulus,
    work_stiffening_modulus,
    entry_flow_stress,
    dilation_factor,
    heat_difference,
    flowing_entry_flags,
    starting_permanent_deformation,
    starting_weights,
    applied_reduced_vector,
    approx_tangent_inverse,
):
    rows, points = starting_permanent_deformation.shape
    own_rows = starting_weights.shape[0]
    size = lax.axis_size
    entries = M * points * size("load")
    place = lax.axis_index(VOX).reshape(1)
    core = lax.axis_index("core").reshape(1)
    load = lax.axis_index("load").reshape(1)
    exchange = functools.partial(lax.all_to_all, split_axis=0, concat_axis=0, tiled=True)

    (weights,) = call(send_kernel, "send", [((size(VOX), own_rows, points), F32)], 3, 1)(
        place, core, load, starting_weights
    )
    xi = exchange(weights, VOX).reshape(CHUNKS, CHUNK, points)

    square = (8, rows // 8)
    wide = ((rows, points), F32)
    fixed = call(
        prepare_kernel,
        "prepare",
        [((M, rows), BF16), ((M, points), F32), ((128, 128), F32), ((1, points), F32), ((rows, points), BF16)],
        1,
        10,
        [pltpu.VMEM((128, points), F32)],
    )(
        place,
        approx_tangent_inverse,
        reduced_shape_matrix,
        young_modulus.reshape(square),
        work_stiffening_modulus.reshape(square),
        entry_flow_stress.reshape(square),
        dilation_factor.reshape(square),
        heat_difference.reshape(1, points),
        flowing_entry_flags,
        applied_reduced_vector,
        starting_permanent_deformation,
    )
    plastic = starting_permanent_deformation
    stress_room = pltpu.VMEM((rows, points), BF16)
    sums_shape = ((M, points), F32)
    xi_shape = ((CHUNKS, CHUNK, points), F32)

    mine = other = None
    for sweep in range(ITERS):
        if sweep == 0:
            plastic, sums = call(first_kernel, "first", [wide, sums_shape], 0, 8, [stress_room])(
                xi, reduced_shape_matrix, *fixed, plastic
            )
        else:
            plastic, sums, xi = call(
                functools.partial(next_kernel, entries),
                "next",
                [wide, sums_shape, xi_shape],
                1,
                10,
                [stress_room, pltpu.VMEM(xi_shape[0], BF16)],
            )(core, mine, other, xi, reduced_shape_matrix, *fixed, plastic)
        pieces = exchange(sums.reshape(CHUNKS, CHUNK, points), COLUMNS)
        (ring,) = call(relay_kernel, "relay", [((size(RING), CHUNK, points), F32)], 0, 1)(pieces)
        ring = exchange(ring, RING)
        (message,) = call(close_kernel, "close", [((size(PLANE), CHUNK + 8, points), F32)], 1, 1)(load, ring)
        mine = exchange(message, PLANE)
        other = lax.ppermute(mine, "core", SWAP)
    (xi_own,) = call(
        functools.partial(last_kernel, entries), "last", [((own_rows, points), F32)], 2, 3
    )(core, place, mine, other, xi)
    return (xi_own, plastic)


def solution(mesh):
    split = Mesh(
        mesh.devices.reshape(4, 2, 4, 2, mesh.shape["load"]),
        ("x", "zl", "y", "core", "load"),
    )
    return jax.shard_map(
        shards,
        mesh=split,
        in_specs=(
            P(VOX, None),
            P(VOX),
            P(VOX),
            P(VOX),
            P(VOX),
            P("load"),
            P(VOX, "load"),
            P(VOX, "load"),
            P(VOX, "load"),
            P(VOX, "load"),
            P(),
        ),
        out_specs=(P(VOX, "load"), P(VOX, "load")),
        check_vma=False,
    )
```

```python
import functools

import jax
import jax.numpy as jnp
from jax import lax
from jax.experimental import pallas as pl
from jax.experimental.pallas import tpu as pltpu
from jax.sharding import Mesh
from jax.sharding import PartitionSpec as P

M = 512
ITERS = 3
VOX = ("x", "zl", "y", "core")
PLANE = ("y", "x")
COLUMNS = ("core", "y", "x")
RING = ("zl", "load")
SWAP = [(0, 1), (1, 0)]
CHUNK = 16
CHUNKS = M // CHUNK
BLOCK = 128

HERE = pl.BlockSpec(memory_space=pltpu.VMEM)
SCALAR = pl.BlockSpec(memory_space=pltpu.SMEM)
F32 = jnp.float32
BF16 = jnp.bfloat16


def call(kernel, name, outs, n_scalars, n_arrays, scratch=(), stay=False):
    return pl.pallas_call(
        kernel,
        name=name,
        out_shape=[(pltpu.VMEM if stay else jax.ShapeDtypeStruct)(*out) for out in outs],
        in_specs=[SCALAR] * n_scalars + [HERE] * n_arrays,
        out_specs=[HERE] * len(outs),
        scratch_shapes=list(scratch),
        compiler_params=pltpu.CompilerParams(vmem_limit_bytes=16 << 20),
    )


def dot(a, b, dims=((1,), (0,))):
    return lax.dot_general(a, b, (dims, ((), ())), preferred_element_type=F32)


def split_two(value):
    high = value.astype(BF16)
    return high, (value - high.astype(F32)).astype(BF16)


def send_kernel(place, core, load, own, out):
    for peer in range(out.shape[0]):
        out[peer] = own[...]


def prepare_kernel(
    place, inverse, basis, young, harden, flow, dilate, heat, flags, applied, plastic,
    map_out, applied_out, columns_out, heat_out, active_out,
    padded,
):
    inverse_high, inverse_low = split_two(inverse[...])
    for block in range(0, basis.shape[0], 256):
        rows = slice(block, block + 256)
        part = basis[rows, :]
        both = dot(inverse_high, part, ((1,), (1,))) + dot(inverse_low, part, ((1,), (1,)))
        map_out[:, rows] = both.astype(BF16)
    heat_out[...] = heat[...]
    active_out[...] = flags[...].astype(BF16)
    padded[...] = jnp.zeros_like(padded)
    padded[pl.ds(pl.multiple_of(place[0] % 16 * 8, 8), 8), :] = applied[...]
    columns = inverse[:, pl.ds(pl.multiple_of(place[0] // 16 * 128, 128), 128)]
    a_high, a_low = split_two(columns)
    b_high, b_low = split_two(padded[...])
    applied_out[...] = dot(a_high, b_high) + (dot(a_high, b_low) + dot(a_low, b_high))
    factors = (
        young[...] / flow[...],
        flow[...],
        young[...],
        flow[...] / (young[...] + harden[...]),
        dilate[...],
    )
    spare = jnp.zeros((128 - 8 * len(factors), 128), F32)
    columns_out[...] = jnp.concatenate([*factors, spare], axis=0).T


def factor_of(mine, other, entries):
    squares = mine[0, CHUNK:] + other[0, CHUNK:]
    for peer in range(1, mine.shape[0]):
        squares = squares + mine[peer, CHUNK:] + other[peer, CHUNK:]
    spread = jnp.sum(squares, axis=(0, 1), keepdims=True) / entries
    return 1.0 / (1.0 + spread)


def constitutive(xi_now, basis, map_in, applied, columns, heat, active, plastic, plastic_out, sums_out, stress_all):
    for block in range(basis.shape[0] // BLOCK):
        rows = slice(block * BLOCK, block * BLOCK + BLOCK)
        slope, flow, young, weight, dilate = (
            columns[:, 8 * factor + block : 8 * factor + block + 1] for factor in range(5)
        )
        strain = dot(basis[rows, :], xi_now)
        ratio = slope * (strain - dilate * heat[...] - plastic[rows, :])
        increment = active[rows, :].astype(F32) * weight * (ratio - jnp.tanh(ratio))
        plastic_out[rows, :] = plastic[rows, :] + increment
        stress_all[rows, :] = (flow * ratio - young * increment).astype(BF16)
    sums_out[...] = dot(map_in[...], stress_all[...]) - applied[...]


def first_kernel(xi, *rest):
    constitutive(xi[...].reshape(M, -1).astype(BF16), *rest)


def next_kernel(entries, core_ref, mine, other, xi, *rest):
    *rest, xi_out, stress_all, xi_low = rest
    core = core_ref[0]
    factor = factor_of(mine, other, entries)
    peers = mine.shape[0]
    for peer in range(peers):
        for source, spot in ((mine, peers * core + peer), (other, peers * (1 - core) + peer)):
            value = xi[spot] - source[peer, :CHUNK] * factor
            xi_out[spot] = value
            xi_low[spot] = value.astype(BF16)
    constitutive(xi_low[...].reshape(M, -1), *rest, stress_all)


def last_kernel(entries, core_ref, place, mine, other, xi, out):
    factor = factor_of(mine, other, entries)
    chunk = place[0] // 2
    half = pl.ds(pl.multiple_of(place[0] % 2 * 8, 8), 8)
    peer = chunk % mine.shape[0]
    here = chunk // mine.shape[0] == core_ref[0]
    delta = jnp.where(here, mine[peer, half], other[peer, half])
    out[...] = xi[chunk, half] - delta * factor


def relay_kernel(pieces, out):
    total = pieces[0]
    for peer in range(1, pieces.shape[0]):
        total = total + pieces[peer]
    for peer in range(out.shape[0]):
        out[peer] = total


def close_kernel(load, pieces, out):
    loads = pieces.shape[0] // 2
    squares = jnp.zeros((8, out.shape[2]), F32)
    for group in range(loads):
        total = pieces[group] + pieces[loads + group]
        square = total * total
        squares = squares + square[:8] + square[8:]
    delta = pieces[load[0]] + pieces[loads + load[0]]
    for peer in range(out.shape[0]):
        out[peer, :CHUNK] = delta
        out[peer, CHUNK:] = squares


def shards(
    reduced_shape_matrix,
    young_modulus,
    work_stiffening_modulus,
    entry_flow_stress,
    dilation_factor,
    heat_difference,
    flowing_entry_flags,
    starting_permanent_deformation,
    starting_weights,
    applied_reduced_vector,
    approx_tangent_inverse,
):
    rows, points = starting_permanent_deformation.shape
    own_rows = starting_weights.shape[0]
    size = lax.axis_size
    entries = M * points * size("load")
    place = lax.axis_index(VOX).reshape(1)
    core = lax.axis_index("core").reshape(1)
    load = lax.axis_index("load").reshape(1)
    exchange = functools.partial(lax.all_to_all, split_axis=0, concat_axis=0, tiled=True)

    (weights,) = call(send_kernel, "send", [((size(VOX), own_rows, points), F32)], 3, 1)(
        place, core, load, starting_weights
    )
    xi = exchange(weights, VOX).reshape(CHUNKS, CHUNK, points)

    square = (8, rows // 8)
    wide = ((rows, points), F32)
    fixed = call(
        prepare_kernel,
        "prepare",
        [((M, rows), BF16), ((M, points), F32), ((128, 128), F32), ((1, points), F32), ((rows, points), BF16)],
        1,
        10,
        [pltpu.VMEM((128, points), F32)],
    )(
        place,
        approx_tangent_inverse,
        reduced_shape_matrix,
        young_modulus.reshape(square),
        work_stiffening_modulus.reshape(square),
        entry_flow_stress.reshape(square),
        dilation_factor.reshape(square),
        heat_difference.reshape(1, points),
        flowing_entry_flags,
        applied_reduced_vector,
        starting_permanent_deformation,
    )
    plastic = starting_permanent_deformation
    stress_room = pltpu.VMEM((rows, points), BF16)
    sums_shape = ((M, points), F32)
    xi_shape = ((CHUNKS, CHUNK, points), F32)

    mine = other = None
    for sweep in range(ITERS):
        if sweep == 0:
            plastic, sums = call(first_kernel, "first", [wide, sums_shape], 0, 8, [stress_room])(
                xi, reduced_shape_matrix, *fixed, plastic
            )
        else:
            plastic, sums, xi = call(
                functools.partial(next_kernel, entries),
                "next",
                [wide, sums_shape, xi_shape],
                1,
                10,
                [stress_room, pltpu.VMEM(xi_shape[0], BF16)],
                True,
            )(core, mine, other, xi, reduced_shape_matrix, *fixed, plastic)
        pieces = exchange(sums.reshape(CHUNKS, CHUNK, points), COLUMNS)
        (ring,) = call(relay_kernel, "relay", [((size(RING), CHUNK, points), F32)], 0, 1)(pieces)
        ring = exchange(ring, RING)
        (message,) = call(close_kernel, "close", [((size(PLANE), CHUNK + 8, points), F32)], 1, 1)(load, ring)
        mine = exchange(message, PLANE)
        other = lax.ppermute(mine, "core", SWAP)
    (xi_own,) = call(
        functools.partial(last_kernel, entries), "last", [((own_rows, points), F32)], 2, 3
    )(core, place, mine, other, xi)
    return (xi_own, plastic)


def solution(mesh):
    split = Mesh(
        mesh.devices.reshape(4, 2, 4, 2, mesh.shape["load"]),
        ("x", "zl", "y", "core", "load"),
    )
    return jax.shard_map(
        shards,
        mesh=split,
        in_specs=(
            P(VOX, None),
            P(VOX),
            P(VOX),
            P(VOX),
            P(VOX),
            P("load"),
            P(VOX, "load"),
            P(VOX, "load"),
            P(VOX, "load"),
            P(VOX, "load"),
            P(),
        ),
        out_specs=(P(VOX, "load"), P(VOX, "load")),
        check_vma=False,
    )
```
